768 devices in a mesh: lat: 16 (over y_lo, x), lon: 48 (over y_hi, z, core).
Axes of the slice: x: 4, y: 8 (y_hi: 2, y_lo: 4; y = y_hi * 4 + y_lo), z: 12, core: 2. Of those that a mesh axis runs over, the one named last changes fastest.
Arguments:
- grid_state: float32 [192, 720, 384], P('lat', 'lon'), may hold values from -6 to 6
- norm_gain: float32 [2, 384], replicated, may hold values from 0.25 to 1.75
- conv_weight: bfloat16 [2, 3, 3, 384, 384], replicated, may hold values from -0.109375 to 0.109375
- filter_weight: bfloat16 [192, 384, 384], P('lat'), may hold values from -0.3125 to 0.3125
- degree_keep: int32 [192, 192], P('lat', 'lon'), may hold values 0 or 1
Outputs:
- updated: float32 [192, 720, 384], P('lat', 'lon')
The draws below stay inside these ranges and needn't reach their ends.
Inputs may be any that keep to these rules, and one draw needn't show every extreme that they name: degree_keep[l, m] is 0 or 1 for degree l and order m.
All inputs are finite; a program needn't handle non-finite values. No bound on the sum of `degree_keep` on one device may be relied on, other than what follows from the above.
Results may differ from the reference program's by a relative error of at most 0.008.
Values may be sent and summed in bfloat16 or wider, within the bound.
No kernel may reach another device: no remote copies, remote signals or barrier semaphores. Data moves between devices by JAX's collectives and lax.ppermute only.
A program may use at most 64 MiB of HBM per device.

```python
import math
import jax
import jax.numpy as jnp
from jax import lax

C = 384
NLAT = 192
NLON = 720
DEGREES = 192


def place_ends(drawn, own_key, smallest, high):
    longest = drawn.shape.index(max(drawn.shape))
    spots = []
    for shift in (0, 1):
        where = [jax.random.randint(jax.random.fold_in(own_key, axis), (), 0, length) for axis, length in enumerate(drawn.shape)]
        where[longest] = (where[longest] + shift) % drawn.shape[longest]
        spots.append(tuple(where))
    return drawn.at[spots[0]].set(smallest).at[spots[1]].set(high)


def steps_of(own_key, dims, shards, smallest, top_value):
    level = 1.0
    for position, blocks in shards:
        draws = jax.random.uniform(jax.random.fold_in(jax.random.fold_in(own_key, 6), position), (blocks,), jnp.float32, smallest / len(shards), top_value / len(shards))
        level = level * jnp.repeat(jnp.exp(draws), dims[position] // blocks).reshape((-1,) + (1,) * (len(dims) - 1 - position))
    return level


def gaussian(stream_key, dims, width, limit, pieces=(), held_as=jnp.bfloat16):
    factor_of = steps_of(stream_key, dims, pieces, -0.22, 0.18) if pieces else 1.0
    array = jax.random.normal(stream_key, dims, jnp.float32) * width * factor_of
    return jnp.minimum(jnp.maximum(array, -limit), limit).astype(held_as)


def setup_inputs(seed: int = 0) -> dict:
    key_of = jax.random.split(jax.random.key(seed), 6)
    grid_state = gaussian(key_of[0], (NLAT, NLON, C), 1.0, 6.0, ((0, 16), (1, 48)), jnp.float32)
    norm_gain = jnp.clip(1.0 + 0.15 * jax.random.normal(key_of[1], (2, C), jnp.float32), 0.25, 1.75)
    conv_weight = gaussian(key_of[2], (2, 3, 3, C, C), (9 * C) ** -0.5, 0.109375)
    filter_weight = gaussian(key_of[3], (DEGREES, C, C), C ** -0.5, 0.3125, ((0, 16),))
    degree_keep = place_ends((jax.random.randint(key_of[4], (DEGREES, DEGREES), 0, 4) < 3).astype(jnp.int32), jax.random.fold_in(key_of[4], 1), 0, 1)
    return {"grid_state": grid_state, "norm_gain": norm_gain, "conv_weight": conv_weight, "filter_weight": filter_weight, "degree_keep": degree_keep}


epsilon = 1e-06

def colatitude(row_index, total_rows, float_type):
    theta_rows = (row_index.astype(float_type) + 0.5) * (math.pi / total_rows)
    return (jnp.cos(theta_rows), jnp.sin(theta_rows))

def legendre_table(orders, cosine, sine_values, amount):
    float_type = cosine.dtype
    order_f = orders.astype(float_type)[:, None]
    order_i = orders.astype(jnp.int32)[:, None]
    column = cosine[None, :]
    log_start = 0.5 * (jnp.log((2.0 * order_f + 1.0) / (4.0 * math.pi)) + jax.scipy.special.gammaln(order_f + 0.5) - jax.scipy.special.gammaln(order_f + 1.0) - 0.5 * math.log(math.pi)) + order_f * jnp.log(sine_values)[None, :]
    sectoral = jnp.exp(log_start)

    def advance(carry, degree):
        before, latest = carry
        degree_f = degree.astype(float_type)
        growth = jnp.sqrt(jnp.maximum(4.0 * degree_f * degree_f - 1.0, 1.0) / jnp.maximum(degree_f * degree_f - order_f * order_f, 1.0))
        prior = degree_f - 1.0
        damping = jnp.sqrt(jnp.maximum(prior * prior - order_f * order_f, 0.0) / jnp.maximum(4.0 * prior * prior - 1.0, 1.0))
        grown = growth * (column * latest - damping * before)
        fresh = jnp.where(degree < order_i, jnp.zeros_like(grown), jnp.where(degree == order_i, sectoral, grown)).astype(float_type)
        return ((latest, fresh), fresh)
    zero_rows = jnp.zeros((orders.shape[0], cosine.shape[0]), float_type)
    _, assoc_basis = lax.scan(advance, (zero_rows, zero_rows), jnp.arange(amount, dtype=jnp.int32), unroll=16)
    return assoc_basis

def forward_table(columns, modes, total_cols, float_type):
    lon_index = columns.astype(jnp.int32)[:, None]
    order_index = jnp.arange(modes, dtype=jnp.int32)[None, :]
    phase = (lon_index * order_index % total_cols).astype(float_type) * (2.0 * math.pi / total_cols)
    factor = 2.0 * math.pi / total_cols
    return jnp.stack([jnp.cos(phase) * factor, -jnp.sin(phase) * factor], axis=2).reshape(columns.shape[0], 2 * modes)

def inverse_table(modes, total_cols, float_type):
    order_index = jnp.arange(modes, dtype=jnp.int32)[:, None]
    lon_index = jnp.arange(total_cols, dtype=jnp.int32)[None, :]
    phase = (lon_index * order_index % total_cols).astype(float_type) * (2.0 * math.pi / total_cols)
    factor = jnp.where(order_index == 0, 1.0, 2.0).astype(float_type)
    return jnp.stack([jnp.cos(phase) * factor, -jnp.sin(phase) * factor], axis=1).reshape(2 * modes, total_cols)

def reference(grid_state, norm_gain, conv_weight, filter_weight, degree_keep):
    hp = lax.Precision.HIGHEST
    float_type = grid_state.dtype
    channels = grid_state.shape[2]
    for depth_index in range(2):
        scale_rows = lax.rsqrt(lax.optimization_barrier(jnp.mean(grid_state * grid_state, axis=-1, keepdims=True)) + epsilon)
        normed = (grid_state * scale_rows * norm_gain[depth_index]).astype(jnp.bfloat16)
        wrapped = jnp.concatenate([normed[:, -1:], normed, normed[:, :1]], axis=1)
        padded = jnp.pad(wrapped, ((1, 1), (0, 0), (0, 0)))
        running = jnp.zeros((NLAT * NLON, channels), jnp.float32)
        for row_tap in range(3):
            for col_tap in range(3):
                window = padded[row_tap:row_tap + NLAT, col_tap:col_tap + NLON].reshape(NLAT * NLON, channels)
                running = running + jnp.dot(window, conv_weight[depth_index, row_tap, col_tap], preferred_element_type=jnp.float32)
        grid_state = grid_state + jax.nn.gelu(running.reshape(NLAT, NLON, channels).astype(float_type), approximate=False)
    rounded = lax.optimization_barrier(grid_state.astype(jnp.bfloat16))
    dft_table = forward_table(jnp.arange(NLON), DEGREES, NLON, float_type)
    spectrum = jnp.einsum('alc,lk->akc', rounded.astype(float_type), dft_table, precision=hp).astype(jnp.bfloat16)
    cosine, sine_values = colatitude(jnp.arange(NLAT), NLAT, float_type)
    assoc_basis = legendre_table(jnp.arange(DEGREES), cosine, sine_values, DEGREES)
    weighted = assoc_basis * (sine_values * (math.pi / NLAT))[None, None, :]
    values = lax.optimization_barrier(spectrum).astype(float_type).reshape(NLAT, DEGREES, 2, channels)
    coefficients = jnp.einsum('lmi,impc->lmpc', weighted, values, precision=hp).reshape(DEGREES, 2 * DEGREES, channels).astype(jnp.bfloat16)
    coefficients = lax.optimization_barrier(coefficients)
    mixing = jnp.einsum('lkc,lcd->lkd', coefficients.astype(float_type), filter_weight.astype(float_type), precision=hp)
    keep_mask = degree_keep.astype(float_type)
    filtered = (mixing.reshape(DEGREES, DEGREES, 2, channels) * keep_mask[:, :, None, None]).astype(jnp.bfloat16)
    filtered = lax.optimization_barrier(filtered)
    synthesis = jnp.einsum('lmi,lmpc->impc', assoc_basis, filtered.astype(float_type), precision=hp).reshape(NLAT, 2 * DEGREES, channels).astype(jnp.bfloat16)
    synthesis = lax.optimization_barrier(synthesis)
    physical = jnp.einsum('akc,kl->alc', synthesis.astype(float_type), inverse_table(DEGREES, NLON, float_type), precision=hp).astype(jnp.bfloat16)
    physical = lax.optimization_barrier(physical)
    return grid_state + jax.nn.gelu(physical.astype(float_type), approximate=False)
```

```python
import functools
import math

import jax
import jax.numpy as jnp
import numpy as np
from jax import lax
from jax.experimental import pallas as pl
from jax.experimental.pallas import tpu as pltpu
from jax.sharding import PartitionSpec as P

EPS = 1e-06
C = 384
LANES = 128
THIRDS = 3
ROWS, COLS = 12, 15
PAD = 16
LAT, LON = 16, 48
NLAT, NLON = 192, 720
MODES = 192
OWN = 4
F32, BF16 = jnp.float32, jnp.bfloat16


def lon_tables():
    m = (OWN * np.arange(LON)[:, None, None] + np.arange(OWN)[None, None, :]) + np.zeros((1, 2, 1), int)
    part = np.zeros((LON, 1, OWN), int) + np.arange(2)[None, :, None]
    m, part = m.reshape(-1), part.reshape(-1)
    j = COLS * np.arange(LON)[:, None] + np.arange(PAD)[None, :]
    held = np.broadcast_to(np.arange(PAD)[None, :] < COLS, j.shape).reshape(-1)
    j = j.reshape(-1)
    phase = (m[:, None] * j[None, :] % NLON) * (2.0 * math.pi / NLON)
    wave = np.where(part[:, None] == 0, np.cos(phase), -np.sin(phase)) * held[None, :]
    forward = wave * (2.0 * math.pi / NLON)
    inverse = (wave * np.where(m == 0, 1.0, 2.0)[:, None]).T
    return jnp.asarray(forward, BF16), jnp.asarray(inverse, BF16)


def padded_rows(values):
    blocks = values.reshape(*values.shape[:-1], LAT, ROWS)
    spare = [(0, 0)] * (blocks.ndim - 1) + [(0, PAD - ROWS)]
    return np.pad(blocks, spare).reshape(*values.shape[:-1], LAT * PAD)


def lat_tables():
    m = np.arange(MODES)[:, None].astype(np.float64)
    l = np.arange(MODES)[None, :].astype(np.float64)
    growth = np.sqrt(np.maximum(4 * l * l - 1, 1) / np.maximum(l * l - m * m, 1))
    prior = l - 1
    damping = np.sqrt(np.maximum(prior * prior - m * m, 0) / np.maximum(4 * prior * prior - 1, 1))
    theta = (np.arange(NLAT) + 0.5) * (math.pi / NLAT)
    gam = np.array([math.lgamma(k + 0.5) - math.lgamma(k + 1.0) for k in range(MODES)])[:, None]
    log_start = 0.5 * (np.log((2 * m + 1) / (4 * math.pi)) + gam - 0.5 * math.log(math.pi))
    sectoral = np.exp(log_start + m * np.log(np.sin(theta))[None, :])
    cosine = padded_rows(np.cos(theta)[None, :])
    weight = padded_rows((np.sin(theta) * (math.pi / NLAT))[None, :])
    return (
        np.stack([growth, damping], 1).astype(np.float32),
        padded_rows(sectoral)[:, None, :].astype(np.float32),
        np.concatenate([cosine, weight], 0).astype(np.float32),
    )


def gelu(value):
    return 0.5 * value * (1.0 + lax.erf(value * math.sqrt(0.5)))


def legendre_kernel(order_ref, coeff_ref, start_ref, rows_ref, weighted_ref, turned_ref, table):
    order = order_ref[0]
    cosine = rows_ref[0:1, :]
    start = start_ref[...]
    table[...] = jnp.zeros_like(table)

    def block(step, carry):
        before, latest = carry
        for inner in range(ROWS):
            degree = step * ROWS + inner
            grown = coeff_ref[0, degree] * (cosine * latest - coeff_ref[1, degree] * before)
            fresh = jnp.where(
                degree < order, jnp.zeros_like(grown), jnp.where(degree == order, start, grown)
            )
            table[pl.ds(step * PAD + inner, 1), :] = fresh
            before, latest = latest, fresh
        return before, latest

    zero = jnp.zeros_like(start)
    lax.fori_loop(0, LAT, block, (zero, zero))
    values = table[...]
    weighted_ref[...] = (values * rows_ref[1:2, :]).astype(BF16)
    turned_ref[...] = values.T.astype(BF16)


def legendre(order):
    coefficients, starts, rows = lat_tables()
    coefficient = lax.dynamic_index_in_dim(jnp.asarray(coefficients), order, 0, False)
    start = lax.dynamic_index_in_dim(jnp.asarray(starts), order, 0, False)
    side = LAT * PAD
    return pl.pallas_call(
        legendre_kernel,
        name="legendre",
        out_shape=[jax.ShapeDtypeStruct((side, side), BF16)] * 2,
        in_specs=[
            pl.BlockSpec(memory_space=pltpu.SMEM),
            pl.BlockSpec(memory_space=pltpu.SMEM),
            pl.BlockSpec(memory_space=pltpu.VMEM),
            pl.BlockSpec(memory_space=pltpu.VMEM),
        ],
        out_specs=[pl.BlockSpec(memory_space=pltpu.VMEM)] * 2,
        scratch_shapes=[pltpu.VMEM((side, side), F32)],
        cost_estimate=pl.CostEstimate(flops=6_000_000, bytes_accessed=300_000, transcendentals=0),
    )(order[None], coefficient, start, jnp.asarray(rows))


def conv_kernel(
    place_ref, x_ref, top_ref, bottom_ref, left_ref, right_ref, gain_ref, weight_ref,
    held_ref, send_ref,
    raw, normed, taps, weights, mid, sems,
):
    copies = []
    for layer in range(2):
        for col in range(3):
            for row in range(3):
                copy = pltpu.make_async_copy(
                    weight_ref.at[layer, row, col],
                    weights.at[layer, col, pl.ds(row * C, C)],
                    sems.at[layer, col, row],
                )
                copy.start()
                copies.append(copy)

    def place_line(start, count, line):
        for third in range(THIRDS):
            raw[third, pl.ds(start, count, stride=PAD), :] = line[
                :, third * LANES : (third + 1) * LANES
            ]

    def raw_lines(start, count):
        return jnp.concatenate([raw[t, start : start + count, :] for t in range(THIRDS)], axis=1)

    for row in range(ROWS):
        place_line(2 * PAD + row + 2, COLS, x_ref[row])
    for row in range(2):
        place_line(2 * PAD + row, COLS, top_ref[row])
        place_line(2 * PAD + ROWS + 2 + row, COLS, bottom_ref[row])
    for row in range(PAD):
        place_line(row, 2, left_ref[row])
        place_line((2 + COLS) * PAD + row, 2, right_ref[row])

    def scaled(value, layer):
        scale = lax.rsqrt(jnp.mean(value * value, axis=-1, keepdims=True) + EPS)
        return value * scale * gain_ref[layer : layer + 1, :]

    def convolved(layer, count):
        for row in range(3):
            taps[0 : count + 2 * PAD, row * C : (row + 1) * C] = normed[
                row : row + count + 2 * PAD, :
            ].astype(BF16)
        total = None
        for col in range(3):
            for row in range(3):
                copies[(layer * 3 + col) * 3 + row].wait()
            part = jnp.dot(
                taps[col * PAD : col * PAD + count, :],
                weights[layer, col],
                preferred_element_type=F32,
            )
            total = part if total is None else total + part
        return total

    first, second = (COLS + 2) * PAD, COLS * PAD
    tail = jnp.zeros((8, C), F32)
    normed[0 : first + 2 * PAD, :] = scaled(raw_lines(0, first + 2 * PAD), 0)
    normed[first + 2 * PAD : first + 2 * PAD + 8, :] = tail
    mid[...] = raw_lines(PAD + 1, first) + gelu(convolved(0, first))
    row = lax.broadcasted_iota(jnp.int32, (first, 1), 0) % PAD
    outside = ((row == 0) & (place_ref[0] == 0)) | ((row == ROWS + 1) & (place_ref[0] == LAT - 1))
    normed[0:first, :] = jnp.where(outside, 0.0, scaled(mid[...], 1))
    normed[first : first + 8, :] = tail
    last = mid[PAD + 1 : PAD + 1 + second, :] + gelu(convolved(1, second))
    for third in range(THIRDS):
        raw[third, 0:second, :] = last[:, third * LANES : (third + 1) * LANES]
        raw[third, second : second + PAD, :] = jnp.zeros((PAD, LANES), F32)
    for row in range(ROWS):
        for third in range(THIRDS):
            line = raw[third, pl.ds(row, PAD, stride=PAD), :]
            held_ref[row, :, third * LANES : (third + 1) * LANES] = line
            send_ref[row * THIRDS + third] = line.astype(BF16)
    send_ref[ROWS * THIRDS :] = jnp.zeros((LON - ROWS * THIRDS, PAD, LANES), BF16)


def convolutions(place, x, top, bottom, left, right, gain, weight):
    spots = (COLS + 4) * PAD
    vmem = pl.BlockSpec(memory_space=pltpu.VMEM)
    return pl.pallas_call(
        conv_kernel,
        name="convolutions",
        out_shape=[
            jax.ShapeDtypeStruct((ROWS, PAD, C), F32),
            jax.ShapeDtypeStruct((LON, PAD, LANES), BF16),
        ],
        in_specs=[pl.BlockSpec(memory_space=pltpu.SMEM)] + [vmem] * 6 + [pl.BlockSpec(memory_space=pl.ANY)],
        out_specs=[vmem, vmem],
        scratch_shapes=[
            pltpu.VMEM((THIRDS, spots, LANES), F32),
            pltpu.VMEM((spots + 8, C), F32),
            pltpu.VMEM((spots, 3 * C), BF16),
            pltpu.VMEM((2, 3, 3 * C, C), BF16),
            pltpu.VMEM(((COLS + 2) * PAD, C), F32),
            pltpu.SemaphoreType.DMA((2, 3, 3)),
        ],
        cost_estimate=pl.CostEstimate(
            flops=2 * 512 * 9 * C * C, bytes_accessed=6_500_000, transcendentals=200_000
        ),
    )(place[None], x, top, bottom, left, right, gain, weight)


def spread_kernel(in_ref, out_ref, held):
    held[...] = in_ref[...].astype(F32).reshape(LON * 8, LANES)
    for third in range(THIRDS):
        for order in range(OWN):
            parts = [
                held[pl.ds(third * 8 + part * OWN + order, PAD, stride=THIRDS * 8), :].astype(BF16)
                for part in range(2)
            ]
            out_ref[third * OWN + order] = jnp.concatenate(parts, axis=1)
    out_ref[THIRDS * OWN :] = jnp.zeros((LAT - THIRDS * OWN, PAD, 2 * LANES), BF16)


def gather_kernel(in_ref, out_ref, held):
    for third in range(THIRDS):
        for order in range(OWN):
            block = in_ref[third * OWN + order].astype(F32)
            for part in range(2):
                held[pl.ds(third * 8 + part * OWN + order, PAD, stride=THIRDS * 8), :] = block[
                    :, part * LANES : (part + 1) * LANES
                ]
    out_ref[...] = held[...].reshape(LON, 8, LANES).astype(BF16)


def reshuffled(kernel, name, shape, data):
    vmem = pl.BlockSpec(memory_space=pltpu.VMEM)
    return pl.pallas_call(
        kernel,
        name=name,
        out_shape=jax.ShapeDtypeStruct(shape, BF16),
        in_specs=[vmem],
        out_specs=vmem,
        scratch_shapes=[pltpu.VMEM((LON * 8, LANES), F32)],
        cost_estimate=pl.CostEstimate(flops=1_000_000, bytes_accessed=250_000, transcendentals=0),
    )(data)


def filter_kernel(in_ref, keep_ref, weight_ref, out_ref, given, made, weights, sems):
    copies = []
    for degree in range(ROWS):
        copy = pltpu.make_async_copy(weight_ref.at[degree], weights.at[degree], sems.at[degree])
        copy.start()
        copies.append(copy)
    for part in range(2):
        given[part] = (
            in_ref[:, :, part * LANES : (part + 1) * LANES].astype(F32).reshape(LAT * PAD, LANES)
        )
    made[...] = jnp.zeros_like(made)
    for degree in range(ROWS):
        lines = [
            jnp.concatenate(
                [
                    given[part, pl.ds(third * OWN * PAD + degree, OWN, stride=PAD), :]
                    for third in range(THIRDS)
                ],
                axis=1,
            )
            for part in range(2)
        ]
        lines = jnp.concatenate(lines, axis=0).astype(BF16)
        copies[degree].wait()
        mixed = jnp.dot(lines, weights[degree], preferred_element_type=F32)
        for third in range(THIRDS):
            piece = mixed[:, third * LANES : (third + 1) * LANES] * keep_ref[degree]
            for part in range(2):
                made[part, pl.ds(third * OWN * PAD + degree, OWN, stride=PAD), :] = piece[
                    part * OWN : (part + 1) * OWN
                ]
    for part in range(2):
        out_ref[:, :, part * LANES : (part + 1) * LANES] = (
            made[part].reshape(LAT, PAD, LANES).astype(BF16)
        )


def filtered(data, keep, weight):
    vmem = pl.BlockSpec(memory_space=pltpu.VMEM)
    lines = jnp.concatenate([keep, keep], axis=1).astype(F32)[:, :, None]
    lines = jnp.broadcast_to(lines, (ROWS, 2 * OWN, LANES))
    return pl.pallas_call(
        filter_kernel,
        name="filter",
        out_shape=jax.ShapeDtypeStruct(data.shape, BF16),
        in_specs=[vmem, vmem, pl.BlockSpec(memory_space=pl.ANY)],
        out_specs=vmem,
        scratch_shapes=[
            pltpu.VMEM((2, LAT * PAD, LANES), F32),
            pltpu.VMEM((2, LAT * PAD, LANES), F32),
            pltpu.VMEM((ROWS, C, C), BF16),
            pltpu.SemaphoreType.DMA((ROWS,)),
        ],
        cost_estimate=pl.CostEstimate(
            flops=2 * ROWS * 128 * C * C, bytes_accessed=4_000_000, transcendentals=0
        ),
    )(data, lines, weight)


def finish_kernel(held_ref, in_ref, out_ref):
    for row in range(ROWS):
        physical = jnp.concatenate([in_ref[row * THIRDS + t] for t in range(THIRDS)], axis=1)
        value = held_ref[row] + gelu(physical.astype(F32))
        out_ref[row] = value[:COLS]


def finished(held, physical):
    vmem = pl.BlockSpec(memory_space=pltpu.VMEM)
    return pl.pallas_call(
        finish_kernel,
        name="finish",
        out_shape=jax.ShapeDtypeStruct((ROWS, COLS, C), F32),
        in_specs=[vmem, vmem],
        out_specs=vmem,
        cost_estimate=pl.CostEstimate(flops=3_000_000, bytes_accessed=800_000, transcendentals=70_000),
    )(held, physical)


def exchange(data, axis):
    return lax.all_to_all(data, axis, 0, 0, tiled=True)


def matmul(left, right):
    return jnp.dot(left, right, preferred_element_type=F32).astype(BF16)


def halo(x):
    up = [(i, i + 1) for i in range(LAT - 1)]
    down = [(j, i) for i, j in up]
    top = lax.ppermute(x[ROWS - 2 :], "lat", up)
    bottom = lax.ppermute(x[:2], "lat", down)
    east = [(i, (i + 1) % LON) for i in range(LON)]
    west = [(j, i) for i, j in east]
    last = jnp.concatenate([top[:, -2:], x[:, -2:], bottom[:, -2:]], axis=0)
    first = jnp.concatenate([top[:, :2], x[:, :2], bottom[:, :2]], axis=0)
    left = lax.ppermute(last, "lon", east)
    right = lax.ppermute(first, "lon", west)
    return top, bottom, left, right


def per_device(grid_state, norm_gain, conv_weight, filter_weight, degree_keep):
    lat, lon = lax.axis_index("lat"), lax.axis_index("lon")
    side = LAT * PAD
    forward, inverse = lon_tables()
    analysis, synthesis = legendre(lon * OWN + lat % OWN)
    edges = halo(grid_state)
    held, data = convolutions(lat, grid_state, *edges, norm_gain, conv_weight)
    data = exchange(data, "lon").reshape(LON * PAD, LANES)
    data = exchange(matmul(forward, data).reshape(LON, 8, LANES), "lon")
    data = reshuffled(spread_kernel, "spread", (LAT, PAD, 2 * LANES), data)
    data = exchange(data, "lat").reshape(side, 2 * LANES)
    data = exchange(matmul(analysis, data).reshape(LAT, PAD, 2 * LANES), "lat")
    data = filtered(data, degree_keep, filter_weight)
    data = exchange(data, "lat").reshape(side, 2 * LANES)
    data = exchange(matmul(synthesis, data).reshape(LAT, PAD, 2 * LANES), "lat")
    data = reshuffled(gather_kernel, "gather", (LON, 8, LANES), data)
    data = exchange(data, "lon").reshape(LON * 8, LANES)
    data = exchange(matmul(inverse, data).reshape(LON, PAD, LANES), "lon")
    return finished(held, data)


def solution(mesh):
    in_specs = (P("lat", "lon", None), P(), P(), P("lat", None, None), P("lat", "lon"))
    return jax.shard_map(
        per_device, mesh=mesh, in_specs=in_specs, out_specs=P("lat", "lon", None), check_vma=False
    )
```

```python
import functools
import math

import jax
import jax.numpy as jnp
import numpy as np
from jax import lax
from jax.experimental import pallas as pl
from jax.experimental.pallas import tpu as pltpu
from jax.sharding import PartitionSpec as P

EPS = 1e-06
C = 384
LANES = 128
THIRDS = 3
ROWS, COLS = 12, 15
PAD = 16
LAT, LON = 16, 48
NLAT, NLON = 192, 720
MODES = 192
SLOTS = 16
PER = 4
F32, BF16 = jnp.float32, jnp.bfloat16


def lon_of(slot, third):
    return (slot // 8 * 12 + slot // 2 % 4 * THIRDS + third) * 2 + slot % 2


ORDER_GROUPS = [
    [a * LON + lon_of(slot, third) for a in range(LAT) for slot in range(SLOTS)]
    for third in range(THIRDS)
]
DEGREE_GROUPS = [
    [a * LON + lon_of(slot, third) for a in range(LAT) for third in range(THIRDS)]
    for slot in range(SLOTS)
]


def lon_table():
    shape = (LAT, SLOTS, 2)
    m = np.broadcast_to(ROWS * np.arange(SLOTS)[None, :, None] + np.arange(LAT)[:, None, None], shape)
    used = np.broadcast_to(np.arange(LAT)[:, None, None] < ROWS, shape).reshape(-1)
    part = np.broadcast_to(np.arange(2)[None, None, :], shape).reshape(-1)
    m = m.reshape(-1)
    j = COLS * np.arange(LON)[:, None] + np.arange(PAD)[None, :]
    held = np.broadcast_to(np.arange(PAD)[None, :] < COLS, j.shape).reshape(-1)
    j = j.reshape(-1)
    phase = (m[:, None] * j[None, :] % NLON) * (2.0 * math.pi / NLON)
    wave = np.where(part[:, None] == 0, np.cos(phase), -np.sin(phase))
    return jnp.asarray(wave * held[None, :] * used[:, None], BF16)


def padded_rows(values):
    blocks = values.reshape(*values.shape[:-1], LAT, ROWS)
    spare = [(0, 0)] * (blocks.ndim - 1) + [(0, PAD - ROWS)]
    return np.pad(blocks, spare).reshape(*values.shape[:-1], LAT * PAD)


def lat_tables():
    m = np.arange(MODES)[:, None].astype(np.float64)
    l = np.arange(MODES)[None, :].astype(np.float64)
    growth = np.sqrt(np.maximum(4 * l * l - 1, 1) / np.maximum(l * l - m * m, 1))
    prior = l - 1
    damping = np.sqrt(np.maximum(prior * prior - m * m, 0) / np.maximum(4 * prior * prior - 1, 1))
    theta = (np.arange(NLAT) + 0.5) * (math.pi / NLAT)
    gam = np.array([math.lgamma(k + 0.5) - math.lgamma(k + 1.0) for k in range(MODES)])[:, None]
    log_start = 0.5 * (np.log((2 * m + 1) / (4 * math.pi)) + gam - 0.5 * math.log(math.pi))
    sectoral = np.exp(log_start + m * np.log(np.sin(theta))[None, :])
    cosine = padded_rows(np.cos(theta)[None, :])
    weight = padded_rows((np.sin(theta) * (math.pi / NLAT))[None, :])
    spare = [(0, 0), (0, LAT * PAD - MODES)]
    table = np.stack([np.pad(growth, spare), np.pad(damping, spare), padded_rows(sectoral)], 1)
    return table.astype(np.float32), np.concatenate([cosine, weight], 0).astype(np.float32)


def gelu(value):
    return 0.5 * value * (1.0 + lax.erf(value * math.sqrt(0.5)))


def legendre_kernel(order_ref, coeff_ref, start_ref, rows_ref, weighted_ref, turned_ref, table):
    order = order_ref[0]
    cosine = rows_ref[0:1, :]
    start = start_ref[2:3, :]

    def block(step, carry):
        before, latest = carry
        for inner in range(PAD):
            degree = step * PAD + inner
            grown = coeff_ref[0, degree] * (cosine * latest - coeff_ref[1, degree] * before)
            fresh = jnp.where(
                degree < order, jnp.zeros_like(grown), jnp.where(degree == order, start, grown)
            )
            table[pl.ds(degree, 1), :] = fresh
            before, latest = latest, fresh
        return before, latest

    zero = jnp.zeros_like(start)
    lax.fori_loop(0, MODES // PAD, block, (zero, zero))
    values = table[...]
    weighted_ref[...] = (values * rows_ref[1:2, :]).astype(BF16)
    turned_ref[...] = (values.T * jnp.where(order == 0, 1.0, 2.0)).astype(BF16)


def legendre(order):
    tables, rows = lat_tables()
    table = lax.dynamic_index_in_dim(jnp.asarray(tables), order, 0, False)
    side = LAT * PAD
    return pl.pallas_call(
        legendre_kernel,
        name="legendre",
        out_shape=[
            jax.ShapeDtypeStruct((MODES, side), BF16),
            jax.ShapeDtypeStruct((side, MODES), BF16),
        ],
        in_specs=[
            pl.BlockSpec(memory_space=pltpu.SMEM),
            pl.BlockSpec(memory_space=pltpu.SMEM),
            pl.BlockSpec(memory_space=pltpu.VMEM),
            pl.BlockSpec(memory_space=pltpu.VMEM),
        ],
        out_specs=[pl.BlockSpec(memory_space=pltpu.VMEM)] * 2,
        scratch_shapes=[pltpu.VMEM((MODES, side), F32)],
        cost_estimate=pl.CostEstimate(flops=6_000_000, bytes_accessed=300_000, transcendentals=0),
    )(order[None], table, table, jnp.asarray(rows))


def conv_kernel(
    place_ref, x_ref, top_ref, bottom_ref, left_ref, right_ref, keep_ref, gain_ref, weight_ref,
    held_ref, send_ref,
    raw, normed, taps, weights, mid, sems,
):
    copies = []
    for layer in range(2):
        for col in range(3):
            for row in range(3):
                copy = pltpu.make_async_copy(
                    weight_ref.at[layer, row, col],
                    weights.at[layer, col, pl.ds(row * C, C)],
                    sems.at[layer, col, row],
                )
                copy.start()
                copies.append(copy)

    def place_line(start, count, line):
        for third in range(THIRDS):
            raw[third, pl.ds(start, count, stride=PAD), :] = line[
                :, third * LANES : (third + 1) * LANES
            ]

    def raw_lines(start, count):
        return jnp.concatenate([raw[t, start : start + count, :] for t in range(THIRDS)], axis=1)

    for row in range(ROWS):
        place_line(2 * PAD + row + 2, COLS, x_ref[row])
    for row in range(2):
        place_line(2 * PAD + row, COLS, top_ref[row])
        place_line(2 * PAD + ROWS + 2 + row, COLS, bottom_ref[row])
    for row in range(PAD):
        place_line(row, 2, left_ref[row])
        place_line((2 + COLS) * PAD + row, 2, right_ref[row])

    def scaled(value, layer):
        scale = lax.rsqrt(jnp.mean(value * value, axis=-1, keepdims=True) + EPS)
        return value * scale * gain_ref[layer : layer + 1, :]

    def convolved(layer, count):
        for row in range(3):
            taps[0 : count + 2 * PAD, row * C : (row + 1) * C] = normed[
                row : row + count + 2 * PAD, :
            ].astype(BF16)
        total = None
        for col in range(3):
            for row in range(3):
                copies[(layer * 3 + col) * 3 + row].wait()
            part = jnp.dot(
                taps[col * PAD : col * PAD + count, :],
                weights[layer, col],
                preferred_element_type=F32,
            )
            total = part if total is None else total + part
        return total

    first, second = (COLS + 2) * PAD, COLS * PAD
    tail = jnp.zeros((8, C), F32)
    normed[0 : first + 2 * PAD, :] = scaled(raw_lines(0, first + 2 * PAD), 0)
    normed[first + 2 * PAD : first + 2 * PAD + 8, :] = tail
    mid[...] = raw_lines(PAD + 1, first) + gelu(convolved(0, first))
    row = lax.broadcasted_iota(jnp.int32, (first, 1), 0) % PAD
    outside = ((row == 0) & (place_ref[0] == 0)) | ((row == ROWS + 1) & (place_ref[0] == LAT - 1))
    normed[0:first, :] = jnp.where(outside, 0.0, scaled(mid[...], 1))
    normed[first : first + 8, :] = tail
    last = mid[PAD + 1 : PAD + 1 + second, :] + gelu(convolved(1, second))
    for third in range(THIRDS):
        raw[third, 0:second, :] = last[:, third * LANES : (third + 1) * LANES]
        raw[third, second : second + PAD, :] = keep_ref[third]
    carried = lax.broadcasted_iota(jnp.int32, (PAD, LANES), 0) == COLS
    for row in range(SLOTS):
        for third in range(THIRDS):
            line = raw[third, pl.ds(row, PAD, stride=PAD), :]
            if row < ROWS:
                held_ref[row, :, third * LANES : (third + 1) * LANES] = line
            else:
                line = jnp.where(carried, line, 0.0)
            send_ref[lon_of(row, third)] = line.astype(BF16)


def convolutions(place, x, top, bottom, left, right, keep, gain, weight):
    spots = (COLS + 4) * PAD
    vmem = pl.BlockSpec(memory_space=pltpu.VMEM)
    return pl.pallas_call(
        conv_kernel,
        name="convolutions",
        out_shape=[
            jax.ShapeDtypeStruct((ROWS, PAD, C), F32),
            jax.ShapeDtypeStruct((LON, PAD, LANES), BF16),
        ],
        in_specs=[pl.BlockSpec(memory_space=pltpu.SMEM)] + [vmem] * 7 + [pl.BlockSpec(memory_space=pl.ANY)],
        out_specs=[vmem, vmem],
        scratch_shapes=[
            pltpu.VMEM((THIRDS, spots, LANES), F32),
            pltpu.VMEM((spots + 8, C), F32),
            pltpu.VMEM((spots, 3 * C), BF16),
            pltpu.VMEM((2, 3, 3 * C, C), BF16),
            pltpu.VMEM(((COLS + 2) * PAD, C), F32),
            pltpu.SemaphoreType.DMA((2, 3, 3)),
        ],
        cost_estimate=pl.CostEstimate(
            flops=2 * 512 * 9 * C * C, bytes_accessed=6_500_000, transcendentals=200_000
        ),
    )(place[None], x, top, bottom, left, right, keep, gain, weight)


def apart(lines, part, count):
    return lines[pl.ds(part, count, stride=2), :]


def lat_kernel(table_ref, in_ref, out_ref, given, made):
    count, depth = table_ref.shape
    given[...] = in_ref[...].astype(F32)
    table = table_ref[...]
    for part in range(2):
        lines = apart(given, part, depth).astype(BF16)
        made[pl.ds(part, count, stride=2), :] = jnp.dot(table, lines, preferred_element_type=F32)
    out_ref[...] = made[...].astype(BF16)


def lat_sums(name, table, data):
    count, depth = table.shape
    vmem = pl.BlockSpec(memory_space=pltpu.VMEM)
    return pl.pallas_call(
        lat_kernel,
        name=name,
        out_shape=jax.ShapeDtypeStruct((2 * count, LANES), BF16),
        in_specs=[vmem, vmem],
        out_specs=vmem,
        scratch_shapes=[pltpu.VMEM((2 * depth, LANES), F32), pltpu.VMEM((2 * count, LANES), F32)],
        cost_estimate=pl.CostEstimate(
            flops=4 * count * depth * LANES, bytes_accessed=400_000, transcendentals=0
        ),
    )(table, data)


def filter_kernel(first_ref, in_ref, keep_ref, weight_ref, out_ref, given, made, weights, sems):
    first = first_ref[0]
    copies = []
    for degree in range(PER):
        copy = pltpu.make_async_copy(
            weight_ref.at[first + degree], weights.at[degree], sems.at[degree]
        )
        copy.start()
        copies.append(copy)
    kept = jnp.sum(keep_ref[:, COLS : COLS + 1, :].astype(F32), axis=0)
    kept = jnp.broadcast_to(kept, (LANES, LANES)).T
    given[...] = in_ref[...].astype(F32)
    for degree in range(PER):
        lines = [
            jnp.concatenate(
                [
                    given[pl.ds(third * 8 + degree * 2 + part, LAT, stride=THIRDS * 8), :]
                    for third in range(THIRDS)
                ],
                axis=1,
            )
            for part in range(2)
        ]
        lines = jnp.concatenate(lines, axis=0).astype(BF16)
        copies[degree].wait()
        mixed = jnp.dot(lines, weights[degree], preferred_element_type=F32)
        for third in range(THIRDS):
            piece = mixed[:, third * LANES : (third + 1) * LANES]
            piece = piece * kept[degree * 2 * LAT : (degree + 1) * 2 * LAT]
            for part in range(2):
                made[pl.ds(third * 8 + degree * 2 + part, LAT, stride=THIRDS * 8), :] = piece[
                    part * LAT : (part + 1) * LAT
                ]
    out_ref[...] = made[...].astype(BF16)


def filtered(first, data, carried, weight):
    vmem = pl.BlockSpec(memory_space=pltpu.VMEM)
    return pl.pallas_call(
        filter_kernel,
        name="filter",
        out_shape=jax.ShapeDtypeStruct(data.shape, BF16),
        in_specs=[
            pl.BlockSpec(memory_space=pltpu.SMEM), vmem, vmem, pl.BlockSpec(memory_space=pl.ANY)
        ],
        out_specs=vmem,
        scratch_shapes=[
            pltpu.VMEM(data.shape, F32),
            pltpu.VMEM(data.shape, F32),
            pltpu.VMEM((PER, C, C), BF16),
            pltpu.SemaphoreType.DMA((PER,)),
        ],
        cost_estimate=pl.CostEstimate(
            flops=2 * PER * 256 * C * C, bytes_accessed=1_700_000, transcendentals=0
        ),
    )(first[None], data, carried, weight)


def finish_kernel(held_ref, in_ref, out_ref):
    for row in range(ROWS):
        physical = jnp.concatenate([in_ref[lon_of(row, t)] for t in range(THIRDS)], axis=1)
        value = held_ref[row] + gelu(physical.astype(F32))
        out_ref[row] = value[:COLS]


def finished(held, physical):
    vmem = pl.BlockSpec(memory_space=pltpu.VMEM)
    return pl.pallas_call(
        finish_kernel,
        name="finish",
        out_shape=jax.ShapeDtypeStruct((ROWS, COLS, C), F32),
        in_specs=[vmem, vmem],
        out_specs=vmem,
        cost_estimate=pl.CostEstimate(flops=3_000_000, bytes_accessed=800_000, transcendentals=70_000),
    )(held, physical)


def exchange(data, axis, groups=None):
    return lax.all_to_all(data, axis, 0, 0, tiled=True, axis_index_groups=groups)


def by_orders(data):
    data = exchange(data.reshape(LAT * SLOTS, 2, LANES), ("lat", "lon"), ORDER_GROUPS)
    return data.reshape(LAT * SLOTS * 2, LANES)


def by_degrees(data):
    data = exchange(data.reshape(LON, 8, LANES), ("lat", "lon"), DEGREE_GROUPS)
    return data.reshape(LON * 8, LANES)


def by_slots(keep, lon):
    keep = keep.astype(F32).reshape(THIRDS, PER, 1, 1, 4)
    here = (jnp.arange(4) == lon % THIRDS).astype(F32).reshape(1, 1, 1, 4, 1)
    lanes = jnp.broadcast_to(keep * here, (THIRDS, PER, 2, 4, 4)).reshape(THIRDS, 1, LANES)
    slot = (jnp.arange(SLOTS) == lon // THIRDS).astype(F32).reshape(1, SLOTS, 1)
    return lanes * slot


def lon_sums(table, data, dim, factor):
    dims = (((dim,), (0,)), ((), ()))
    return (lax.dot_general(table, data, dims, preferred_element_type=F32) * factor).astype(BF16)


def halo(x):
    up = [(i, i + 1) for i in range(LAT - 1)]
    down = [(j, i) for i, j in up]
    top = lax.ppermute(x[ROWS - 2 :], "lat", up)
    bottom = lax.ppermute(x[:2], "lat", down)
    east = [(i, (i + 1) % LON) for i in range(LON)]
    west = [(j, i) for i, j in east]
    last = jnp.concatenate([top[:, -2:], x[:, -2:], bottom[:, -2:]], axis=0)
    first = jnp.concatenate([top[:, :2], x[:, :2], bottom[:, :2]], axis=0)
    left = lax.ppermute(last, "lon", east)
    right = lax.ppermute(first, "lon", west)
    return top, bottom, left, right


def per_device(grid_state, norm_gain, conv_weight, filter_weight, degree_keep):
    lat, lon = lax.axis_index("lat"), lax.axis_index("lon")
    turn = lon // 2 % 12
    slot, third = lon // 24 * 8 + turn // THIRDS * 2 + lon % 2, turn % THIRDS
    waves = lon_table()
    analysis, synthesis = legendre(jnp.minimum(slot * ROWS + lat, MODES - 1))
    keep = by_slots(degree_keep, lon)
    edges = halo(grid_state)
    held, data = convolutions(lat, grid_state, *edges, keep, norm_gain, conv_weight)
    carried = exchange(data, "lon")
    data = lon_sums(waves, carried.reshape(LON * PAD, LANES), 1, 2.0 * math.pi / NLON)
    data = by_orders(data)
    data = by_degrees(lat_sums("analysis", analysis, data))
    data = by_degrees(filtered(third * PER, data, carried, filter_weight))
    data = by_orders(lat_sums("synthesis", synthesis, data))
    data = exchange(lon_sums(waves, data, 0, 1.0).reshape(LON, PAD, LANES), "lon")
    return finished(held, data)


def solution(mesh):
    in_specs = (P("lat", "lon", None), P(), P(), P("lat", None, None), P("lat", "lon"))
    return jax.shard_map(
        per_device, mesh=mesh, in_specs=in_specs, out_specs=P("lat", "lon", None), check_vma=False
    )
```

```python
import functools
import math

import jax
import jax.numpy as jnp
import numpy as np
from jax import lax
from jax.experimental import pallas as pl
from jax.experimental.pallas import tpu as pltpu
from jax.sharding import PartitionSpec as P

EPS = 1e-06
C = 384
LANES = 128
THIRDS = 3
ROWS, COLS = 12, 15
PAD = 16
LAT, LON = 16, 48
NLAT, NLON = 192, 720
MODES = 192
SLOTS = 16
PER = 4
F32, BF16 = jnp.float32, jnp.bfloat16


def lon_of(slot, third):
    return (slot // 8 * 12 + slot // 2 % 4 * THIRDS + third) * 2 + slot % 2


ORDER_GROUPS = [
    [a * LON + lon_of(slot, third) for a in range(LAT) for slot in range(SLOTS)]
    for third in range(THIRDS)
]
DEGREE_GROUPS = [
    [a * LON + lon_of(slot, third) for a in range(LAT) for third in range(THIRDS)]
    for slot in range(SLOTS)
]


def lon_table():
    shape = (LAT, SLOTS, 2)
    m = np.broadcast_to(ROWS * np.arange(SLOTS)[None, :, None] + np.arange(LAT)[:, None, None], shape)
    used = np.broadcast_to(np.arange(LAT)[:, None, None] < ROWS, shape).reshape(-1)
    part = np.broadcast_to(np.arange(2)[None, None, :], shape).reshape(-1)
    m = m.reshape(-1)
    j = COLS * np.arange(LON)[:, None] + np.arange(PAD)[None, :]
    held = np.broadcast_to(np.arange(PAD)[None, :] < COLS, j.shape).reshape(-1)
    j = j.reshape(-1)
    phase = (m[:, None] * j[None, :] % NLON) * (2.0 * math.pi / NLON)
    wave = np.where(part[:, None] == 0, np.cos(phase), -np.sin(phase))
    return jnp.asarray(wave * held[None, :] * used[:, None], BF16)


def padded_rows(values):
    blocks = values.reshape(*values.shape[:-1], LAT, ROWS)
    spare = [(0, 0)] * (blocks.ndim - 1) + [(0, PAD - ROWS)]
    return np.pad(blocks, spare).reshape(*values.shape[:-1], LAT * PAD)


def lat_tables():
    m = np.arange(MODES)[:, None].astype(np.float64)
    l = np.arange(MODES)[None, :].astype(np.float64)
    growth = np.sqrt(np.maximum(4 * l * l - 1, 1) / np.maximum(l * l - m * m, 1))
    prior = l - 1
    damping = np.sqrt(np.maximum(prior * prior - m * m, 0) / np.maximum(4 * prior * prior - 1, 1))
    theta = (np.arange(NLAT) + 0.5) * (math.pi / NLAT)
    gam = np.array([math.lgamma(k + 0.5) - math.lgamma(k + 1.0) for k in range(MODES)])[:, None]
    log_start = 0.5 * (np.log((2 * m + 1) / (4 * math.pi)) + gam - 0.5 * math.log(math.pi))
    sectoral = np.exp(log_start + m * np.log(np.sin(theta))[None, :])
    cosine = padded_rows(np.cos(theta)[None, :])
    weight = padded_rows((np.sin(theta) * (math.pi / NLAT))[None, :])
    spare = [(0, 0), (0, LAT * PAD - MODES)]
    table = np.stack([np.pad(growth, spare), np.pad(damping, spare), padded_rows(sectoral)], 1)
    return table.astype(np.float32), np.concatenate([cosine, weight], 0).astype(np.float32)


def grant(mebibytes):
    return pltpu.CompilerParams(vmem_limit_bytes=mebibytes * 2**20)


def gelu(value):
    return 0.5 * value * (1.0 + lax.erf(value * math.sqrt(0.5)))


def legendre_kernel(order_ref, coeff_ref, start_ref, rows_ref, weighted_ref, turned_ref, table):
    order = order_ref[0]
    cosine = rows_ref[0:1, :]
    start = start_ref[2:3, :]

    def block(step, carry):
        before, latest = carry
        for inner in range(PAD):
            degree = step * PAD + inner
            grown = coeff_ref[0, degree] * (cosine * latest - coeff_ref[1, degree] * before)
            fresh = jnp.where(
                degree < order, jnp.zeros_like(grown), jnp.where(degree == order, start, grown)
            )
            table[pl.ds(degree, 1), :] = fresh
            before, latest = latest, fresh
        return before, latest

    zero = jnp.zeros_like(start)
    lax.fori_loop(0, MODES // PAD, block, (zero, zero))
    values = table[...]
    weighted_ref[...] = (values * rows_ref[1:2, :]).astype(BF16)
    turned_ref[...] = (values.T * jnp.where(order == 0, 1.0, 2.0)).astype(BF16)


def legendre(order):
    tables, rows = lat_tables()
    table = lax.dynamic_index_in_dim(jnp.asarray(tables), order, 0, False)
    side = LAT * PAD
    return pl.pallas_call(
        legendre_kernel,
        name="legendre",
        compiler_params=grant(6),
        out_shape=[
            jax.ShapeDtypeStruct((MODES, side), BF16),
            jax.ShapeDtypeStruct((side, MODES), BF16),
        ],
        in_specs=[
            pl.BlockSpec(memory_space=pltpu.SMEM),
            pl.BlockSpec(memory_space=pltpu.SMEM),
            pl.BlockSpec(memory_space=pltpu.VMEM),
            pl.BlockSpec(memory_space=pltpu.VMEM),
        ],
        out_specs=[pl.BlockSpec(memory_space=pltpu.VMEM)] * 2,
        scratch_shapes=[pltpu.VMEM((MODES, side), F32)],
        cost_estimate=pl.CostEstimate(flops=6_000_000, bytes_accessed=300_000, transcendentals=0),
    )(order[None], table, table, jnp.asarray(rows))


def conv_kernel(
    place_ref, x_ref, top_ref, bottom_ref, left_ref, right_ref, keep_ref, gain_ref, weight_ref,
    held_ref, send_ref,
    raw, normed, taps, weights, mid, sems,
):
    copies = []
    for layer in range(2):
        for col in range(3):
            for row in range(3):
                copy = pltpu.make_async_copy(
                    weight_ref.at[layer, row, col],
                    weights.at[layer, col, pl.ds(row * C, C)],
                    sems.at[layer, col, row],
                )
                copy.start()
                copies.append(copy)

    def place_line(start, count, line):
        for third in range(THIRDS):
            raw[third, pl.ds(start, count, stride=PAD), :] = line[
                :, third * LANES : (third + 1) * LANES
            ]

    def raw_lines(start, count):
        return jnp.concatenate([raw[t, start : start + count, :] for t in range(THIRDS)], axis=1)

    for row in range(ROWS):
        place_line(2 * PAD + row + 2, COLS, x_ref[row])
    for row in range(2):
        place_line(2 * PAD + row, COLS, top_ref[row])
        place_line(2 * PAD + ROWS + 2 + row, COLS, bottom_ref[row])
    for row in range(PAD):
        place_line(row, 2, left_ref[row])
        place_line((2 + COLS) * PAD + row, 2, right_ref[row])

    def scaled(value, layer):
        scale = lax.rsqrt(jnp.mean(value * value, axis=-1, keepdims=True) + EPS)
        return value * scale * gain_ref[layer : layer + 1, :]

    def convolved(layer, count):
        for row in range(3):
            taps[0 : count + 2 * PAD, row * C : (row + 1) * C] = normed[
                row : row + count + 2 * PAD, :
            ].astype(BF16)
        total = None
        for col in range(3):
            for row in range(3):
                copies[(layer * 3 + col) * 3 + row].wait()
            part = jnp.dot(
                taps[col * PAD : col * PAD + count, :],
                weights[layer, col],
                preferred_element_type=F32,
            )
            total = part if total is None else total + part
        return total

    first, second = (COLS + 2) * PAD, COLS * PAD
    tail = jnp.zeros((8, C), F32)
    normed[0 : first + 2 * PAD, :] = scaled(raw_lines(0, first + 2 * PAD), 0)
    normed[first + 2 * PAD : first + 2 * PAD + 8, :] = tail
    mid[...] = raw_lines(PAD + 1, first) + gelu(convolved(0, first))
    row = lax.broadcasted_iota(jnp.int32, (first, 1), 0) % PAD
    outside = ((row == 0) & (place_ref[0] == 0)) | ((row == ROWS + 1) & (place_ref[0] == LAT - 1))
    normed[0:first, :] = jnp.where(outside, 0.0, scaled(mid[...], 1))
    normed[first : first + 8, :] = tail
    last = mid[PAD + 1 : PAD + 1 + second, :] + gelu(convolved(1, second))
    for third in range(THIRDS):
        raw[third, 0:second, :] = last[:, third * LANES : (third + 1) * LANES]
        raw[third, second : second + PAD, :] = keep_ref[third]
    carried = lax.broadcasted_iota(jnp.int32, (PAD, LANES), 0) == COLS
    for row in range(SLOTS):
        for third in range(THIRDS):
            line = raw[third, pl.ds(row, PAD, stride=PAD), :]
            if row < ROWS:
                held_ref[row, :, third * LANES : (third + 1) * LANES] = line
            else:
                line = jnp.where(carried, line, 0.0)
            send_ref[lon_of(row, third)] = line.astype(BF16)


def convolutions(place, x, top, bottom, left, right, keep, gain, weight):
    spots = (COLS + 4) * PAD
    vmem = pl.BlockSpec(memory_space=pltpu.VMEM)
    return pl.pallas_call(
        conv_kernel,
        name="convolutions",
        out_shape=[
            jax.ShapeDtypeStruct((ROWS, PAD, C), F32),
            jax.ShapeDtypeStruct((LON, PAD, LANES), BF16),
        ],
        in_specs=[pl.BlockSpec(memory_space=pltpu.SMEM)] + [vmem] * 7 + [pl.BlockSpec(memory_space=pl.ANY)],
        out_specs=[vmem, vmem],
        scratch_shapes=[
            pltpu.VMEM((THIRDS, spots, LANES), F32),
            pltpu.VMEM((spots + 8, C), F32),
            pltpu.VMEM((spots, 3 * C), BF16),
            pltpu.VMEM((2, 3, 3 * C, C), BF16),
            pltpu.VMEM(((COLS + 2) * PAD, C), F32),
            pltpu.SemaphoreType.DMA((2, 3, 3)),
        ],
        cost_estimate=pl.CostEstimate(
            flops=2 * 512 * 9 * C * C, bytes_accessed=6_500_000, transcendentals=200_000
        ),
    )(place[None], x, top, bottom, left, right, keep, gain, weight)


def apart(lines, part, count):
    return lines[pl.ds(part, count, stride=2), :]


def lat_kernel(table_ref, in_ref, out_ref, given, made):
    count, depth = table_ref.shape
    given[...] = in_ref[...].astype(F32)
    table = table_ref[...]
    for part in range(2):
        lines = apart(given, part, depth).astype(BF16)
        made[pl.ds(part, count, stride=2), :] = jnp.dot(table, lines, preferred_element_type=F32)
    out_ref[...] = made[...].astype(BF16)


def lat_sums(name, table, data):
    count, depth = table.shape
    vmem = pl.BlockSpec(memory_space=pltpu.VMEM)
    return pl.pallas_call(
        lat_kernel,
        name=name,
        compiler_params=grant(6),
        out_shape=jax.ShapeDtypeStruct((2 * count, LANES), BF16),
        in_specs=[vmem, vmem],
        out_specs=vmem,
        scratch_shapes=[pltpu.VMEM((2 * depth, LANES), F32), pltpu.VMEM((2 * count, LANES), F32)],
        cost_estimate=pl.CostEstimate(
            flops=4 * count * depth * LANES, bytes_accessed=400_000, transcendentals=0
        ),
    )(table, data)


def filter_kernel(first_ref, in_ref, keep_ref, weight_ref, out_ref, given, made):
    first = first_ref[0]
    kept = jnp.sum(keep_ref[:, COLS : COLS + 1, :].astype(F32), axis=0)
    kept = jnp.broadcast_to(kept, (LANES, LANES)).T
    given[...] = in_ref[...].astype(F32)
    for degree in range(PER):
        lines = [
            jnp.concatenate(
                [
                    given[pl.ds(third * 8 + degree * 2 + part, LAT, stride=THIRDS * 8), :]
                    for third in range(THIRDS)
                ],
                axis=1,
            )
            for part in range(2)
        ]
        lines = jnp.concatenate(lines, axis=0).astype(BF16)
        mixed = jnp.dot(lines, weight_ref[first + degree], preferred_element_type=F32)
        for third in range(THIRDS):
            piece = mixed[:, third * LANES : (third + 1) * LANES]
            piece = piece * kept[degree * 2 * LAT : (degree + 1) * 2 * LAT]
            for part in range(2):
                made[pl.ds(third * 8 + degree * 2 + part, LAT, stride=THIRDS * 8), :] = piece[
                    part * LAT : (part + 1) * LAT
                ]
    out_ref[...] = made[...].astype(BF16)


def filtered(first, data, carried, weight):
    vmem = pl.BlockSpec(memory_space=pltpu.VMEM)
    return pl.pallas_call(
        filter_kernel,
        name="filter",
        compiler_params=grant(8),
        out_shape=jax.ShapeDtypeStruct(data.shape, BF16),
        in_specs=[pl.BlockSpec(memory_space=pltpu.SMEM), vmem, vmem, vmem],
        out_specs=vmem,
        scratch_shapes=[
            pltpu.VMEM(data.shape, F32),
            pltpu.VMEM(data.shape, F32),
        ],
        cost_estimate=pl.CostEstimate(
            flops=2 * PER * 256 * C * C, bytes_accessed=1_700_000, transcendentals=0
        ),
    )(first[None], data, carried, weight)


def finish_kernel(held_ref, in_ref, out_ref):
    for row in range(ROWS):
        physical = jnp.concatenate([in_ref[lon_of(row, t)] for t in range(THIRDS)], axis=1)
        value = held_ref[row] + gelu(physical.astype(F32))
        out_ref[row] = value[:COLS]


def finished(held, physical):
    vmem = pl.BlockSpec(memory_space=pltpu.VMEM)
    return pl.pallas_call(
        finish_kernel,
        name="finish",
        compiler_params=grant(6),
        out_shape=jax.ShapeDtypeStruct((ROWS, COLS, C), F32),
        in_specs=[vmem, vmem],
        out_specs=vmem,
        cost_estimate=pl.CostEstimate(flops=3_000_000, bytes_accessed=800_000, transcendentals=70_000),
    )(held, physical)


def exchange(data, axis, groups=None):
    return lax.all_to_all(data, axis, 0, 0, tiled=True, axis_index_groups=groups)


def by_orders(data):
    data = exchange(data.reshape(LAT * SLOTS, 2, LANES), ("lat", "lon"), ORDER_GROUPS)
    return data.reshape(LAT * SLOTS * 2, LANES)


def by_degrees(data):
    data = exchange(data.reshape(LON, 8, LANES), ("lat", "lon"), DEGREE_GROUPS)
    return data.reshape(LON * 8, LANES)


def by_slots(keep, lon):
    keep = keep.astype(F32).reshape(THIRDS, PER, 1, 1, 4)
    here = (jnp.arange(4) == lon % THIRDS).astype(F32).reshape(1, 1, 1, 4, 1)
    lanes = jnp.broadcast_to(keep * here, (THIRDS, PER, 2, 4, 4)).reshape(THIRDS, 1, LANES)
    slot = (jnp.arange(SLOTS) == lon // THIRDS).astype(F32).reshape(1, SLOTS, 1)
    return lanes * slot


def lon_sums(table, data, dim, factor):
    dims = (((dim,), (0,)), ((), ()))
    return (lax.dot_general(table, data, dims, preferred_element_type=F32) * factor).astype(BF16)


def lat_halo(x):
    up = [(i, i + 1) for i in range(LAT - 1)]
    down = [(j, i) for i, j in up]
    return lax.ppermute(x[ROWS - 2 :], "lat", up), lax.ppermute(x[:2], "lat", down)


def lon_halo(x, top, bottom):
    east = [(i, (i + 1) % LON) for i in range(LON)]
    west = [(j, i) for i, j in east]
    last = jnp.concatenate([top[:, -2:], x[:, -2:], bottom[:, -2:]], axis=0)
    first = jnp.concatenate([top[:, :2], x[:, :2], bottom[:, :2]], axis=0)
    return lax.ppermute(last, "lon", east), lax.ppermute(first, "lon", west)


def per_device(grid_state, norm_gain, conv_weight, filter_weight, degree_keep):
    lat, lon = lax.axis_index("lat"), lax.axis_index("lon")
    turn = lon // 2 % 12
    slot, third = lon // 24 * 8 + turn // THIRDS * 2 + lon % 2, turn % THIRDS
    waves = lon_table()
    analysis, synthesis = legendre(jnp.minimum(slot * ROWS + lat, MODES - 1))
    keep = by_slots(degree_keep, lon)
    ready = (*lat_halo(grid_state), keep, analysis, synthesis, third * PER)
    top, bottom, keep, analysis, synthesis, degree = lax.optimization_barrier(ready)
    edges = (top, bottom, *lon_halo(grid_state, top, bottom))
    held, data = convolutions(lat, grid_state, *edges, keep, norm_gain, conv_weight)
    carried = exchange(data, "lon")
    data = lon_sums(waves, carried.reshape(LON * PAD, LANES), 1, 2.0 * math.pi / NLON)
    data = by_orders(data)
    data = by_degrees(lat_sums("analysis", analysis, data))
    data = by_degrees(filtered(degree, data, carried, filter_weight))
    data = by_orders(lat_sums("synthesis", synthesis, data))
    data = exchange(lon_sums(waves, data, 0, 1.0).reshape(LON, PAD, LANES), "lon")
    return finished(held, data)


def solution(mesh):
    in_specs = (P("lat", "lon", None), P(), P(), P("lat", None, None), P("lat", "lon"))
    return jax.shard_map(
        per_device, mesh=mesh, in_specs=in_specs, out_specs=P("lat", "lon", None), check_vma=False
    )
```

```python
import functools
import math

import jax
import jax.numpy as jnp
import numpy as np
from jax import lax
from jax.experimental import pallas as pl
from jax.experimental.pallas import tpu as pltpu
from jax.sharding import PartitionSpec as P

EPS = 1e-06
C = 384
LANES = 128
THIRDS = 3
ROWS, COLS = 12, 15
PAD = 16
LAT, LON = 16, 48
NLAT, NLON = 192, 720
MODES = 192
SLOTS = 16
PER = 4
F32, BF16 = jnp.float32, jnp.bfloat16


def lon_of(slot, third):
    return (slot // 8 * 12 + slot // 2 % 4 * THIRDS + third) * 2 + slot % 2


ORDER_GROUPS = [
    [a * LON + lon_of(slot, third) for a in range(LAT) for slot in range(SLOTS)]
    for third in range(THIRDS)
]
DEGREE_GROUPS = [
    [a * LON + lon_of(slot, third) for a in range(LAT) for third in range(THIRDS)]
    for slot in range(SLOTS)
]


def lon_table():
    shape = (LAT, SLOTS, 2)
    m = np.broadcast_to(ROWS * np.arange(SLOTS)[None, :, None] + np.arange(LAT)[:, None, None], shape)
    used = np.broadcast_to(np.arange(LAT)[:, None, None] < ROWS, shape).reshape(-1)
    part = np.broadcast_to(np.arange(2)[None, None, :], shape).reshape(-1)
    m = m.reshape(-1)
    j = COLS * np.arange(LON)[:, None] + np.arange(PAD)[None, :]
    held = np.broadcast_to(np.arange(PAD)[None, :] < COLS, j.shape).reshape(-1)
    j = j.reshape(-1)
    phase = (m[:, None] * j[None, :] % NLON) * (2.0 * math.pi / NLON)
    wave = np.where(part[:, None] == 0, np.cos(phase), -np.sin(phase))
    return jnp.asarray(wave * held[None, :] * used[:, None], BF16)


def padded_rows(values):
    blocks = values.reshape(*values.shape[:-1], LAT, ROWS)
    spare = [(0, 0)] * (blocks.ndim - 1) + [(0, PAD - ROWS)]
    return np.pad(blocks, spare).reshape(*values.shape[:-1], LAT * PAD)


def lat_tables():
    m = np.arange(MODES)[:, None].astype(np.float64)
    l = np.arange(MODES)[None, :].astype(np.float64)
    growth = np.sqrt(np.maximum(4 * l * l - 1, 1) / np.maximum(l * l - m * m, 1))
    prior = l - 1
    damping = np.sqrt(np.maximum(prior * prior - m * m, 0) / np.maximum(4 * prior * prior - 1, 1))
    theta = (np.arange(NLAT) + 0.5) * (math.pi / NLAT)
    gam = np.array([math.lgamma(k + 0.5) - math.lgamma(k + 1.0) for k in range(MODES)])[:, None]
    log_start = 0.5 * (np.log((2 * m + 1) / (4 * math.pi)) + gam - 0.5 * math.log(math.pi))
    sectoral = np.exp(log_start + m * np.log(np.sin(theta))[None, :])
    cosine = padded_rows(np.cos(theta)[None, :])
    weight = padded_rows((np.sin(theta) * (math.pi / NLAT))[None, :])
    spare = [(0, 0), (0, LAT * PAD - MODES)]
    table = np.stack([np.pad(growth, spare), np.pad(damping, spare), padded_rows(sectoral)], 1)
    return table.astype(np.float32), np.concatenate([cosine, weight], 0).astype(np.float32)


def grant(mebibytes):
    return pltpu.CompilerParams(vmem_limit_bytes=mebibytes * 2**20)


def gelu(value):
    return 0.5 * value * (1.0 + lax.erf(value * math.sqrt(0.5)))


def legendre_kernel(order_ref, coeff_ref, start_ref, rows_ref, weighted_ref, turned_ref, table):
    order = order_ref[0]
    cosine = rows_ref[0:1, :]
    start = start_ref[2:3, :]

    def block(step, carry):
        before, latest = carry
        for inner in range(PAD):
            degree = step * PAD + inner
            grown = coeff_ref[0, degree] * (cosine * latest - coeff_ref[1, degree] * before)
            fresh = jnp.where(
                degree < order, jnp.zeros_like(grown), jnp.where(degree == order, start, grown)
            )
            table[pl.ds(degree, 1), :] = fresh
            before, latest = latest, fresh
        return before, latest

    zero = jnp.zeros_like(start)
    lax.fori_loop(0, MODES // PAD, block, (zero, zero))
    values = table[...]
    weighted_ref[...] = (values * rows_ref[1:2, :]).astype(BF16)
    turned_ref[...] = (values.T * jnp.where(order == 0, 1.0, 2.0)).astype(BF16)


def legendre(order):
    tables, rows = lat_tables()
    table = lax.dynamic_index_in_dim(jnp.asarray(tables), order, 0, False)
    side = LAT * PAD
    return pl.pallas_call(
        legendre_kernel,
        name="legendre",
        compiler_params=grant(6),
        out_shape=[
            jax.ShapeDtypeStruct((MODES, side), BF16),
            jax.ShapeDtypeStruct((side, MODES), BF16),
        ],
        in_specs=[
            pl.BlockSpec(memory_space=pltpu.SMEM),
            pl.BlockSpec(memory_space=pltpu.SMEM),
            pl.BlockSpec(memory_space=pltpu.VMEM),
            pl.BlockSpec(memory_space=pltpu.VMEM),
        ],
        out_specs=[pl.BlockSpec(memory_space=pltpu.VMEM)] * 2,
        scratch_shapes=[pltpu.VMEM((MODES, side), F32)],
        cost_estimate=pl.CostEstimate(flops=6_000_000, bytes_accessed=300_000, transcendentals=0),
    )(order[None], table, table, jnp.asarray(rows))


def conv_kernel(
    place_ref, x_ref, top_ref, bottom_ref, left_ref, right_ref, keep_ref, gain_ref, weight_ref,
    held_ref, send_ref,
    raw, normed, taps, weights, mid, sems,
):
    copies = []
    for layer in range(2):
        for col in range(3):
            for row in range(3):
                copy = pltpu.make_async_copy(
                    weight_ref.at[layer, row, col],
                    weights.at[layer, col, pl.ds(row * C, C)],
                    sems.at[layer, col, row],
                )
                copy.start()
                copies.append(copy)

    def place_line(start, count, line):
        for third in range(THIRDS):
            raw[third, pl.ds(start, count, stride=PAD), :] = line[
                :, third * LANES : (third + 1) * LANES
            ]

    def raw_lines(start, count):
        return jnp.concatenate([raw[t, start : start + count, :] for t in range(THIRDS)], axis=1)

    for row in range(ROWS):
        place_line(2 * PAD + row + 2, COLS, x_ref[row])
    for row in range(2):
        place_line(2 * PAD + row, COLS, top_ref[row])
        place_line(2 * PAD + ROWS + 2 + row, COLS, bottom_ref[row])
    for row in range(PAD):
        place_line(row, 2, left_ref[row])
        place_line((2 + COLS) * PAD + row, 2, right_ref[row])

    def scaled(value, layer):
        scale = lax.rsqrt(jnp.mean(value * value, axis=-1, keepdims=True) + EPS)
        return value * scale * gain_ref[layer : layer + 1, :]

    def convolved(layer, count):
        for row in range(3):
            taps[0 : count + 2 * PAD, row * C : (row + 1) * C] = normed[
                row : row + count + 2 * PAD, :
            ].astype(BF16)
        total = None
        for col in range(3):
            for row in range(3):
                copies[(layer * 3 + col) * 3 + row].wait()
            part = jnp.dot(
                taps[col * PAD : col * PAD + count, :],
                weights[layer, col],
                preferred_element_type=F32,
            )
            total = part if total is None else total + part
        return total

    first, second = (COLS + 2) * PAD, COLS * PAD
    tail = jnp.zeros((8, C), F32)
    normed[0 : first + 2 * PAD, :] = scaled(raw_lines(0, first + 2 * PAD), 0)
    normed[first + 2 * PAD : first + 2 * PAD + 8, :] = tail
    mid[...] = raw_lines(PAD + 1, first) + gelu(convolved(0, first))
    row = lax.broadcasted_iota(jnp.int32, (first, 1), 0) % PAD
    outside = ((row == 0) & (place_ref[0] == 0)) | ((row == ROWS + 1) & (place_ref[0] == LAT - 1))
    normed[0:first, :] = jnp.where(outside, 0.0, scaled(mid[...], 1))
    normed[first : first + 8, :] = tail
    last = mid[PAD + 1 : PAD + 1 + second, :] + gelu(convolved(1, second))
    for third in range(THIRDS):
        raw[third, 0:second, :] = last[:, third * LANES : (third + 1) * LANES]
        raw[third, second : second + PAD, :] = keep_ref[third]
    carried = lax.broadcasted_iota(jnp.int32, (PAD, LANES), 0) == COLS
    for row in range(SLOTS):
        for third in range(THIRDS):
            line = raw[third, pl.ds(row, PAD, stride=PAD), :]
            if row < ROWS:
                held_ref[row, :, third * LANES : (third + 1) * LANES] = line
            else:
                line = jnp.where(carried, line, 0.0)
            send_ref[lon_of(row, third)] = line.astype(BF16)


def convolutions(place, x, top, bottom, left, right, keep, gain, weight):
    spots = (COLS + 4) * PAD
    vmem = pl.BlockSpec(memory_space=pltpu.VMEM)
    return pl.pallas_call(
        conv_kernel,
        name="convolutions",
        out_shape=[
            jax.ShapeDtypeStruct((ROWS, PAD, C), F32),
            jax.ShapeDtypeStruct((LON, PAD, LANES), BF16),
        ],
        in_specs=[pl.BlockSpec(memory_space=pltpu.SMEM)] + [vmem] * 7 + [pl.BlockSpec(memory_space=pl.ANY)],
        out_specs=[vmem, vmem],
        scratch_shapes=[
            pltpu.VMEM((THIRDS, spots, LANES), F32),
            pltpu.VMEM((spots + 8, C), F32),
            pltpu.VMEM((spots, 3 * C), BF16),
            pltpu.VMEM((2, 3, 3 * C, C), BF16),
            pltpu.VMEM(((COLS + 2) * PAD, C), F32),
            pltpu.SemaphoreType.DMA((2, 3, 3)),
        ],
        cost_estimate=pl.CostEstimate(
            flops=2 * 512 * 9 * C * C, bytes_accessed=6_500_000, transcendentals=200_000
        ),
    )(place[None], x, top, bottom, left, right, keep, gain, weight)


def apart(lines, part, count):
    return lines[pl.ds(part, count, stride=2), :]


def lat_kernel(table_ref, in_ref, out_ref, given, made):
    count, depth = table_ref.shape
    given[...] = in_ref[...].astype(F32)
    table = table_ref[...]
    for part in range(2):
        lines = apart(given, part, depth).astype(BF16)
        made[pl.ds(part, count, stride=2), :] = jnp.dot(table, lines, preferred_element_type=F32)
    out_ref[...] = made[...].astype(BF16)


def lat_sums(name, table, data):
    count, depth = table.shape
    vmem = pl.BlockSpec(memory_space=pltpu.VMEM)
    return pl.pallas_call(
        lat_kernel,
        name=name,
        compiler_params=grant(6),
        out_shape=jax.ShapeDtypeStruct((2 * count, LANES), BF16),
        in_specs=[vmem, vmem],
        out_specs=vmem,
        scratch_shapes=[pltpu.VMEM((2 * depth, LANES), F32), pltpu.VMEM((2 * count, LANES), F32)],
        cost_estimate=pl.CostEstimate(
            flops=4 * count * depth * LANES, bytes_accessed=400_000, transcendentals=0
        ),
    )(table, data)


def filter_kernel(first_ref, in_ref, keep_ref, weight_ref, out_ref, given, made, weights, sems):
    first = first_ref[0]
    copies = []
    for degree in range(PER):
        copy = pltpu.make_async_copy(
            weight_ref.at[first + degree], weights.at[degree], sems.at[degree]
        )
        copy.start()
        copies.append(copy)
    kept = jnp.sum(keep_ref[:, COLS : COLS + 1, :].astype(F32), axis=0)
    kept = jnp.broadcast_to(kept, (LANES, LANES)).T
    given[...] = in_ref[...].astype(F32)
    for degree in range(PER):
        lines = [
            jnp.concatenate(
                [
                    given[pl.ds(third * 8 + degree * 2 + part, LAT, stride=THIRDS * 8), :]
                    for third in range(THIRDS)
                ],
                axis=1,
            )
            for part in range(2)
        ]
        lines = jnp.concatenate(lines, axis=0).astype(BF16)
        copies[degree].wait()
        mixed = jnp.dot(lines, weights[degree], preferred_element_type=F32)
        for third in range(THIRDS):
            piece = mixed[:, third * LANES : (third + 1) * LANES]
            piece = piece * kept[degree * 2 * LAT : (degree + 1) * 2 * LAT]
            for part in range(2):
                made[pl.ds(third * 8 + degree * 2 + part, LAT, stride=THIRDS * 8), :] = piece[
                    part * LAT : (part + 1) * LAT
                ]
    out_ref[...] = made[...].astype(BF16)


def filtered(first, data, carried, weight):
    vmem = pl.BlockSpec(memory_space=pltpu.VMEM)
    return pl.pallas_call(
        filter_kernel,
        name="filter",
        compiler_params=grant(61),
        out_shape=jax.ShapeDtypeStruct(data.shape, BF16),
        in_specs=[
            pl.BlockSpec(memory_space=pltpu.SMEM), vmem, vmem, pl.BlockSpec(memory_space=pl.ANY)
        ],
        out_specs=vmem,
        scratch_shapes=[
            pltpu.VMEM(data.shape, F32),
            pltpu.VMEM(data.shape, F32),
            pltpu.VMEM((PER, C, C), BF16),
            pltpu.SemaphoreType.DMA((PER,)),
        ],
        cost_estimate=pl.CostEstimate(
            flops=2 * PER * 256 * C * C, bytes_accessed=1_700_000, transcendentals=0
        ),
    )(first[None], data, carried, weight)


def finish_kernel(held_ref, in_ref, out_ref):
    for row in range(ROWS):
        physical = jnp.concatenate([in_ref[lon_of(row, t)] for t in range(THIRDS)], axis=1)
        value = held_ref[row] + gelu(physical.astype(F32))
        out_ref[row] = value[:COLS]


def finished(held, physical):
    vmem = pl.BlockSpec(memory_space=pltpu.VMEM)
    return pl.pallas_call(
        finish_kernel,
        name="finish",
        compiler_params=grant(6),
        out_shape=jax.ShapeDtypeStruct((ROWS, COLS, C), F32),
        in_specs=[vmem, vmem],
        out_specs=vmem,
        cost_estimate=pl.CostEstimate(flops=3_000_000, bytes_accessed=800_000, transcendentals=70_000),
    )(held, physical)


def exchange(data, axis, groups=None):
    return lax.all_to_all(data, axis, 0, 0, tiled=True, axis_index_groups=groups)


def by_orders(data):
    data = exchange(data.reshape(LAT * SLOTS, 2, LANES), ("lat", "lon"), ORDER_GROUPS)
    return data.reshape(LAT * SLOTS * 2, LANES)


def by_degrees(data):
    data = exchange(data.reshape(LON, 8, LANES), ("lat", "lon"), DEGREE_GROUPS)
    return data.reshape(LON * 8, LANES)


def by_slots(keep, lon):
    keep = keep.astype(F32).reshape(THIRDS, PER, 1, 1, 4)
    here = (jnp.arange(4) == lon % THIRDS).astype(F32).reshape(1, 1, 1, 4, 1)
    lanes = jnp.broadcast_to(keep * here, (THIRDS, PER, 2, 4, 4)).reshape(THIRDS, 1, LANES)
    slot = (jnp.arange(SLOTS) == lon // THIRDS).astype(F32).reshape(1, SLOTS, 1)
    return lanes * slot


def lon_sums(table, data, dim, factor):
    dims = (((dim,), (0,)), ((), ()))
    return (lax.dot_general(table, data, dims, preferred_element_type=F32) * factor).astype(BF16)


def lat_halo(x):
    up = [(i, i + 1) for i in range(LAT - 1)]
    down = [(j, i) for i, j in up]
    return lax.ppermute(x[ROWS - 2 :], "lat", up), lax.ppermute(x[:2], "lat", down)


def lon_halo(x, top, bottom):
    east = [(i, (i + 1) % LON) for i in range(LON)]
    west = [(j, i) for i, j in east]
    last = jnp.concatenate([top[:, -2:], x[:, -2:], bottom[:, -2:]], axis=0)
    first = jnp.concatenate([top[:, :2], x[:, :2], bottom[:, :2]], axis=0)
    return lax.ppermute(last, "lon", east), lax.ppermute(first, "lon", west)


def per_device(grid_state, norm_gain, conv_weight, filter_weight, degree_keep):
    lat, lon = lax.axis_index("lat"), lax.axis_index("lon")
    turn = lon // 2 % 12
    slot, third = lon // 24 * 8 + turn // THIRDS * 2 + lon % 2, turn % THIRDS
    waves = lon_table()
    analysis, synthesis = legendre(jnp.minimum(slot * ROWS + lat, MODES - 1))
    keep = by_slots(degree_keep, lon)
    top, bottom = lat_halo(grid_state)
    top, bottom, degree = lax.optimization_barrier((top, bottom, third * PER))
    edges = (top, bottom, *lon_halo(grid_state, top, bottom))
    held, data = convolutions(lat, grid_state, *edges, keep, norm_gain, conv_weight)
    carried = exchange(data, "lon")
    data = lon_sums(waves, carried.reshape(LON * PAD, LANES), 1, 2.0 * math.pi / NLON)
    data = by_orders(data)
    data = by_degrees(lat_sums("analysis", analysis, data))
    data = by_degrees(filtered(degree, data, carried, filter_weight))
    data = by_orders(lat_sums("synthesis", synthesis, data))
    data = exchange(lon_sums(waves, data, 0, 1.0).reshape(LON, PAD, LANES), "lon")
    return finished(held, data)


def solution(mesh):
    in_specs = (P("lat", "lon", None), P(), P(), P("lat", None, None), P("lat", "lon"))
    return jax.shard_map(
        per_device, mesh=mesh, in_specs=in_specs, out_specs=P("lat", "lon", None), check_vma=False
    )
```

```python
import math

import jax
import jax.numpy as jnp
import numpy as np
from jax import lax
from jax.experimental import pallas as pl
from jax.experimental.pallas import tpu as pltpu
from jax.sharding import PartitionSpec as P


EPS = 1e-06
C = 384
LANES = 128
THIRDS = 3
ROWS, COLS = 12, 15
PAD = 16
LAT, LON = 16, 48
NLAT, NLON = 192, 720
MODES = 192
SLOTS = 16
PER = 4
F32, BF16 = jnp.float32, jnp.bfloat16


def lon_of(slot, third):
    return (slot // 8 * 12 + slot // 2 % 4 * THIRDS + third) * 2 + slot % 2


ORDER_GROUPS = [
    [a * LON + lon_of(slot, third) for a in range(LAT) for slot in range(SLOTS)]
    for third in range(THIRDS)
]
DEGREE_GROUPS = [
    [a * LON + lon_of(slot, third) for a in range(LAT) for third in range(THIRDS)]
    for slot in range(SLOTS)
]


def lon_table():
    shape = (LAT, SLOTS, 2)
    m = np.broadcast_to(ROWS * np.arange(SLOTS)[None, :, None] + np.arange(LAT)[:, None, None], shape)
    used = np.broadcast_to(np.arange(LAT)[:, None, None] < ROWS, shape).reshape(-1)
    part = np.broadcast_to(np.arange(2)[None, None, :], shape).reshape(-1)
    m = m.reshape(-1)
    j = COLS * np.arange(LON)[:, None] + np.arange(PAD)[None, :]
    held = np.broadcast_to(np.arange(PAD)[None, :] < COLS, j.shape).reshape(-1)
    j = j.reshape(-1)
    phase = (m[:, None] * j[None, :] % NLON) * (2.0 * math.pi / NLON)
    wave = np.where(part[:, None] == 0, np.cos(phase), -np.sin(phase))
    return jnp.asarray(wave * held[None, :] * used[:, None], BF16)


def padded_rows(values):
    blocks = values.reshape(*values.shape[:-1], LAT, ROWS)
    spare = [(0, 0)] * (blocks.ndim - 1) + [(0, PAD - ROWS)]
    return np.pad(blocks, spare).reshape(*values.shape[:-1], LAT * PAD)


def lat_tables():
    m = np.arange(MODES)[:, None].astype(np.float64)
    l = np.arange(MODES)[None, :].astype(np.float64)
    growth = np.sqrt(np.maximum(4 * l * l - 1, 1) / np.maximum(l * l - m * m, 1))
    prior = l - 1
    damping = np.sqrt(np.maximum(prior * prior - m * m, 0) / np.maximum(4 * prior * prior - 1, 1))
    theta = (np.arange(NLAT) + 0.5) * (math.pi / NLAT)
    gam = np.array([math.lgamma(k + 0.5) - math.lgamma(k + 1.0) for k in range(MODES)])[:, None]
    log_start = 0.5 * (np.log((2 * m + 1) / (4 * math.pi)) + gam - 0.5 * math.log(math.pi))
    sectoral = np.exp(log_start + m * np.log(np.sin(theta))[None, :])
    cosine = padded_rows(np.cos(theta)[None, :])
    weight = padded_rows((np.sin(theta) * (math.pi / NLAT))[None, :])
    spare = [(0, 0), (0, LAT * PAD - MODES)]
    table = np.stack([np.pad(growth, spare), np.pad(damping, spare), padded_rows(sectoral)], 1)
    return table.astype(np.float32), np.concatenate([cosine, weight], 0).astype(np.float32)


def grant(mebibytes):
    return pltpu.CompilerParams(vmem_limit_bytes=mebibytes * 2**20)


def gelu(value):
    return 0.5 * value * (1.0 + lax.erf(value * math.sqrt(0.5)))


def legendre_kernel(order_ref, coeff_ref, start_ref, rows_ref, weighted_ref, turned_ref, table):
    order = order_ref[0]
    cosine = rows_ref[0:1, :]
    start = start_ref[2:3, :]

    def block(step, carry):
        before, latest = carry
        for inner in range(PAD):
            degree = step * PAD + inner
            grown = coeff_ref[0, degree] * (cosine * latest - coeff_ref[1, degree] * before)
            fresh = jnp.where(
                degree < order, jnp.zeros_like(grown), jnp.where(degree == order, start, grown)
            )
            table[pl.ds(degree, 1), :] = fresh
            before, latest = latest, fresh
        return before, latest

    zero = jnp.zeros_like(start)
    lax.fori_loop(0, MODES // PAD, block, (zero, zero))
    values = table[...]
    weighted_ref[...] = (values * rows_ref[1:2, :]).astype(BF16)
    turned_ref[...] = (values.T * jnp.where(order == 0, 1.0, 2.0)).astype(BF16)


def legendre(order):
    tables, rows = lat_tables()
    table = lax.dynamic_index_in_dim(jnp.asarray(tables), order, 0, False)
    side = LAT * PAD
    return pl.pallas_call(
        legendre_kernel,
        name="legendre",
        compiler_params=grant(6),
        out_shape=[
            jax.ShapeDtypeStruct((MODES, side), BF16),
            jax.ShapeDtypeStruct((side, MODES), BF16),
        ],
        in_specs=[
            pl.BlockSpec(memory_space=pltpu.SMEM),
            pl.BlockSpec(memory_space=pltpu.SMEM),
            pl.BlockSpec(memory_space=pltpu.VMEM),
            pl.BlockSpec(memory_space=pltpu.VMEM),
        ],
        out_specs=[pl.BlockSpec(memory_space=pltpu.VMEM)] * 2,
        scratch_shapes=[pltpu.VMEM((MODES, side), F32)],
        cost_estimate=pl.CostEstimate(flops=6_000_000, bytes_accessed=300_000, transcendentals=0),
    )(order[None], table, table, jnp.asarray(rows))


def conv_kernel(
    place_ref, x_ref, top_ref, bottom_ref, left_ref, right_ref, keep_ref, gain_ref, weight_ref,
    held_ref, send_ref,
    raw, normed, taps, weights, mid, sems,
):
    copies = []
    for layer in range(2):
        for col in range(3):
            for row in range(3):
                copy = pltpu.make_async_copy(
                    weight_ref.at[layer, row, col],
                    weights.at[layer, col, pl.ds(row * C, C)],
                    sems.at[layer, col, row],
                )
                copy.start()
                copies.append(copy)

    def place_line(start, count, line):
        for third in range(THIRDS):
            raw[third, pl.ds(start, count, stride=PAD), :] = line[
                :, third * LANES : (third + 1) * LANES
            ]

    def raw_lines(start, count):
        return jnp.concatenate([raw[t, start : start + count, :] for t in range(THIRDS)], axis=1)

    for row in range(ROWS):
        place_line(2 * PAD + row + 2, COLS, x_ref[row])
    for row in range(2):
        place_line(2 * PAD + row, COLS, top_ref[row])
        place_line(2 * PAD + ROWS + 2 + row, COLS, bottom_ref[row])
    for row in range(PAD):
        place_line(row, 2, left_ref[row])
        place_line((2 + COLS) * PAD + row, 2, right_ref[row])

    def scaled(value, layer):
        scale = lax.rsqrt(jnp.mean(value * value, axis=-1, keepdims=True) + EPS)
        return value * scale * gain_ref[layer : layer + 1, :]

    def convolved(layer, count):
        for row in range(3):
            taps[0 : count + 2 * PAD, row * C : (row + 1) * C] = normed[
                row : row + count + 2 * PAD, :
            ].astype(BF16)
        total = None
        for col in range(3):
            for row in range(3):
                copies[(layer * 3 + col) * 3 + row].wait()
            part = jnp.dot(
                taps[col * PAD : col * PAD + count, :],
                weights[layer, col],
                preferred_element_type=F32,
            )
            total = part if total is None else total + part
        return total

    first, second = (COLS + 2) * PAD, COLS * PAD
    tail = jnp.zeros((8, C), F32)
    normed[0 : first + 2 * PAD, :] = scaled(raw_lines(0, first + 2 * PAD), 0)
    normed[first + 2 * PAD : first + 2 * PAD + 8, :] = tail
    mid[...] = raw_lines(PAD + 1, first) + gelu(convolved(0, first))
    row = lax.broadcasted_iota(jnp.int32, (first, 1), 0) % PAD
    outside = ((row == 0) & (place_ref[0] == 0)) | ((row == ROWS + 1) & (place_ref[0] == LAT - 1))
    normed[0:first, :] = jnp.where(outside, 0.0, scaled(mid[...], 1))
    normed[first : first + 8, :] = tail
    last = mid[PAD + 1 : PAD + 1 + second, :] + gelu(convolved(1, second))
    for third in range(THIRDS):
        raw[third, 0:second, :] = last[:, third * LANES : (third + 1) * LANES]
        raw[third, second : second + PAD, :] = keep_ref[third]
    carried = lax.broadcasted_iota(jnp.int32, (PAD, LANES), 0) == COLS
    for row in range(SLOTS):
        for third in range(THIRDS):
            line = raw[third, pl.ds(row, PAD, stride=PAD), :]
            if row < ROWS:
                held_ref[row, :, third * LANES : (third + 1) * LANES] = line
            else:
                line = jnp.where(carried, line, 0.0)
            send_ref[lon_of(row, third)] = line.astype(BF16)


def convolutions(place, x, top, bottom, left, right, keep, gain, weight):
    spots = (COLS + 4) * PAD
    vmem = pl.BlockSpec(memory_space=pltpu.VMEM)
    return pl.pallas_call(
        conv_kernel,
        name="convolutions",
        out_shape=[
            jax.ShapeDtypeStruct((ROWS, PAD, C), F32),
            jax.ShapeDtypeStruct((LON, PAD, LANES), BF16),
        ],
        in_specs=[pl.BlockSpec(memory_space=pltpu.SMEM)] + [vmem] * 7 + [pl.BlockSpec(memory_space=pl.ANY)],
        out_specs=[vmem, vmem],
        scratch_shapes=[
            pltpu.VMEM((THIRDS, spots, LANES), F32),
            pltpu.VMEM((spots + 8, C), F32),
            pltpu.VMEM((spots, 3 * C), BF16),
            pltpu.VMEM((2, 3, 3 * C, C), BF16),
            pltpu.VMEM(((COLS + 2) * PAD, C), F32),
            pltpu.SemaphoreType.DMA((2, 3, 3)),
        ],
        cost_estimate=pl.CostEstimate(
            flops=2 * 512 * 9 * C * C, bytes_accessed=6_500_000, transcendentals=200_000
        ),
    )(place[None], x, top, bottom, left, right, keep, gain, weight)


def apart(lines, part, count):
    return lines[pl.ds(part, count, stride=2), :]


def lat_kernel(table_ref, in_ref, out_ref, given, made):
    count, depth = table_ref.shape
    given[...] = in_ref[...].astype(F32)
    table = table_ref[...]
    for part in range(2):
        lines = apart(given, part, depth).astype(BF16)
        made[pl.ds(part, count, stride=2), :] = jnp.dot(table, lines, preferred_element_type=F32)
    out_ref[...] = made[...].astype(BF16)


def lat_sums(table, data):
    count, depth = table.shape
    vmem = pl.BlockSpec(memory_space=pltpu.VMEM)
    return pl.pallas_call(
        lat_kernel,
        compiler_params=grant(6),
        out_shape=jax.ShapeDtypeStruct((2 * count, LANES), BF16),
        in_specs=[vmem, vmem],
        out_specs=vmem,
        scratch_shapes=[pltpu.VMEM((2 * depth, LANES), F32), pltpu.VMEM((2 * count, LANES), F32)],
        cost_estimate=pl.CostEstimate(
            flops=4 * count * depth * LANES, bytes_accessed=400_000, transcendentals=0
        ),
    )(table, data)


def filter_kernel(first_ref, in_ref, keep_ref, weight_ref, out_ref, given, made, weights, sems):
    first = first_ref[0]
    copies = []
    for degree in range(PER):
        copy = pltpu.make_async_copy(
            weight_ref.at[first + degree], weights.at[degree], sems.at[degree]
        )
        copy.start()
        copies.append(copy)
    kept = jnp.sum(keep_ref[:, COLS : COLS + 1, :].astype(F32), axis=0)
    kept = jnp.broadcast_to(kept, (LANES, LANES)).T
    given[...] = in_ref[...].astype(F32)
    for degree in range(PER):
        lines = [
            jnp.concatenate(
                [
                    given[pl.ds(third * 8 + degree * 2 + part, LAT, stride=THIRDS * 8), :]
                    for third in range(THIRDS)
                ],
                axis=1,
            )
            for part in range(2)
        ]
        lines = jnp.concatenate(lines, axis=0).astype(BF16)
        copies[degree].wait()
        mixed = jnp.dot(lines, weights[degree], preferred_element_type=F32)
        for third in range(THIRDS):
            piece = mixed[:, third * LANES : (third + 1) * LANES]
            piece = piece * kept[degree * 2 * LAT : (degree + 1) * 2 * LAT]
            for part in range(2):
                made[pl.ds(third * 8 + degree * 2 + part, LAT, stride=THIRDS * 8), :] = piece[
                    part * LAT : (part + 1) * LAT
                ]
    out_ref[...] = made[...].astype(BF16)


def filtered(first, data, carried, weight):
    vmem = pl.BlockSpec(memory_space=pltpu.VMEM)
    return pl.pallas_call(
        filter_kernel,
        name="filter",
        compiler_params=grant(61),
        out_shape=jax.ShapeDtypeStruct(data.shape, BF16),
        in_specs=[
            pl.BlockSpec(memory_space=pltpu.SMEM), vmem, vmem, pl.BlockSpec(memory_space=pl.ANY)
        ],
        out_specs=vmem,
        scratch_shapes=[
            pltpu.VMEM(data.shape, F32),
            pltpu.VMEM(data.shape, F32),
            pltpu.VMEM((PER, C, C), BF16),
            pltpu.SemaphoreType.DMA((PER,)),
        ],
        cost_estimate=pl.CostEstimate(
            flops=2 * PER * 256 * C * C, bytes_accessed=1_700_000, transcendentals=0
        ),
    )(first[None], data, carried, weight)


def finish_kernel(held_ref, in_ref, out_ref):
    for row in range(ROWS):
        physical = jnp.concatenate([in_ref[lon_of(row, t)] for t in range(THIRDS)], axis=1)
        value = held_ref[row] + gelu(physical.astype(F32))
        out_ref[row] = value[:COLS]


def finished(held, physical):
    vmem = pl.BlockSpec(memory_space=pltpu.VMEM)
    return pl.pallas_call(
        finish_kernel,
        name="finish",
        compiler_params=grant(6),
        out_shape=jax.ShapeDtypeStruct((ROWS, COLS, C), F32),
        in_specs=[vmem, vmem],
        out_specs=vmem,
        cost_estimate=pl.CostEstimate(flops=3_000_000, bytes_accessed=800_000, transcendentals=70_000),
    )(held, physical)


def exchange(data, axis, groups=None):
    return lax.all_to_all(data, axis, 0, 0, tiled=True, axis_index_groups=groups)


def by_orders(data):
    data = exchange(data.reshape(LAT * SLOTS, 2, LANES), ("lat", "lon"), ORDER_GROUPS)
    return data.reshape(LAT * SLOTS * 2, LANES)


def by_degrees(data):
    data = exchange(data.reshape(LON, 8, LANES), ("lat", "lon"), DEGREE_GROUPS)
    return data.reshape(LON * 8, LANES)


def by_slots(keep, lon):
    keep = keep.astype(F32).reshape(THIRDS, PER, 1, 1, 4)
    here = (jnp.arange(4) == lon % THIRDS).astype(F32).reshape(1, 1, 1, 4, 1)
    lanes = jnp.broadcast_to(keep * here, (THIRDS, PER, 2, 4, 4)).reshape(THIRDS, 1, LANES)
    slot = (jnp.arange(SLOTS) == lon // THIRDS).astype(F32).reshape(1, SLOTS, 1)
    return lanes * slot


def lon_sums(table, data, dim, factor):
    dims = (((dim,), (0,)), ((), ()))
    return (lax.dot_general(table, data, dims, preferred_element_type=F32) * factor).astype(BF16)


def lat_halo(x):
    up = [(i, i + 1) for i in range(LAT - 1)]
    down = [(j, i) for i, j in up]
    return lax.ppermute(x[ROWS - 2 :], "lat", up), lax.ppermute(x[:2], "lat", down)


def lon_halo(x, top, bottom):
    east = [(i, (i + 1) % LON) for i in range(LON)]
    west = [(j, i) for i, j in east]
    last = jnp.concatenate([top[:, -2:], x[:, -2:], bottom[:, -2:]], axis=0)
    first = jnp.concatenate([top[:, :2], x[:, :2], bottom[:, :2]], axis=0)
    left = lax.ppermute(last, "lon", east)
    right = lax.ppermute(first, "lon", west)
    return left, right


def per_device(grid_state, norm_gain, conv_weight, filter_weight, degree_keep):
    lat, lon = lax.axis_index("lat"), lax.axis_index("lon")
    turn = lon // 2 % 12
    slot, third = lon // 24 * 8 + turn // THIRDS * 2 + lon % 2, turn % THIRDS
    waves = lon_table()
    analysis, synthesis = legendre(jnp.minimum(slot * ROWS + lat, MODES - 1))
    keep = by_slots(degree_keep, lon)
    top, bottom = lat_halo(grid_state)
    top, bottom, degree = lax.optimization_barrier((top, bottom, third * PER))
    edges = (top, bottom, *lon_halo(grid_state, top, bottom))
    held, data = convolutions(lat, grid_state, *edges, keep, norm_gain, conv_weight)
    carried = exchange(data, "lon")
    data = lon_sums(waves, carried.reshape(LON * PAD, LANES), 1, 2.0 * math.pi / NLON)
    data = by_orders(data)
    data = by_degrees(lat_sums(analysis, data))
    data = by_degrees(filtered(degree, data, carried, filter_weight))
    data = by_orders(lat_sums(synthesis, data))
    data = exchange(lon_sums(waves, data, 0, 1.0).reshape(LON, PAD, LANES), "lon")
    return finished(held, data)


def solution(mesh):
    in_specs = (P("lat", "lon", None), P(), P(), P("lat", None, None), P("lat", "lon"))
    return jax.shard_map(
        per_device, mesh=mesh, in_specs=in_specs, out_specs=P("lat", "lon", None), check_vma=False
    )
```
